32 devices in a mesh: rep: 8 (over z, core), tp: 4 (over y, x).
Axes of the slice: x: 2, y: 2, z: 4, core: 2. Of those that a mesh axis runs over, the one named last changes fastest.
Arguments:
- delta_query: bfloat16 [8, 2, 2048, 3072], P('rep', None, None, 'tp'), may hold values from -6 to 6
- master_query: float32 [2, 2048, 3072], P(None, 'rep', 'tp'), may hold values from -3 to 3
- moment_query: float32 [2, 2048, 3072], P(None, 'rep', 'tp'), may hold values from -3 to 3
- delta_latent: bfloat16 [8, 2, 512, 4096], P('rep', None, None, 'tp'), may hold values from -6 to 6
- master_latent: float32 [2, 512, 4096], P(None, 'rep', 'tp'), may hold values from -3 to 3
- moment_latent: float32 [2, 512, 4096], P(None, 'rep', 'tp'), may hold values from -3 to 3
- delta_output: bfloat16 [8, 2, 2048, 2048], P('rep', None, 'tp'), may hold values from -6 to 6
- master_output: float32 [2, 2048, 2048], P(None, 'tp', 'rep'), may hold values from -3 to 3
- moment_output: float32 [2, 2048, 2048], P(None, 'tp', 'rep'), may hold values from -3 to 3
Outputs:
- params_query: bfloat16 [2, 2048, 3072], P(None, None, 'tp')
- new_master_query: float32 [2, 2048, 3072], P(None, 'rep', 'tp')
- new_moment_query: float32 [2, 2048, 3072], P(None, 'rep', 'tp')
- params_latent: bfloat16 [2, 512, 4096], P(None, None, 'tp')
- new_master_latent: float32 [2, 512, 4096], P(None, 'rep', 'tp')
- new_moment_latent: float32 [2, 512, 4096], P(None, 'rep', 'tp')
- params_output: bfloat16 [2, 2048, 2048], P(None, 'tp')
- new_master_output: float32 [2, 2048, 2048], P(None, 'tp', 'rep')
- new_moment_output: float32 [2, 2048, 2048], P(None, 'tp', 'rep')
The draws below stay inside these ranges and needn't reach their ends.
All inputs are finite; a program needn't handle non-finite values.
Results may differ from the reference program's by a relative error of at most 0.012.
Values may be sent and summed in bfloat16 or wider, within the bound.
A program may use at most 128 MiB of HBM per device.

```python
import jax
import jax.numpy as jnp
from jax import lax

D = 2048
KV_RANK = 512
LAYERS = 2
REPLICAS = 8
QCOLS = 3072
KVCOLS = 4096
OROWS = 2048


def spiked(drawn, rng, source, target, blocks, factor):
    owner, partner = [(jnp.arange(drawn.shape[dim]) // (drawn.shape[dim] // blocks)).reshape([-1 if axis == dim else 1 for axis in range(drawn.ndim)]) for dim in (source, target)]
    chosen = jax.random.permutation(rng, blocks)[partner]
    strong = (owner == chosen) | (owner == (partner + blocks // 2) % blocks)
    return jnp.where(strong, factor * drawn, drawn)


def level_of(own_key, dims, pieces, smallest, top_value):
    loudness = 1.0
    for dim, parts in pieces:
        steps = jax.random.uniform(jax.random.fold_in(jax.random.fold_in(own_key, 6), dim), (parts,), jnp.float32, smallest / len(pieces), top_value / len(pieces))
        loudness = loudness * jnp.repeat(jnp.exp(steps), dims[dim] // parts).reshape((-1,) + (1,) * (len(dims) - 1 - dim))
    return loudness


def gaussian(own_key, extent, scale, bound, shards=(), kind=jnp.bfloat16):
    drawn = jax.random.normal(own_key, extent, jnp.float32) * scale
    if len(shards) > 0:
        drawn = level_of(own_key, extent, shards, -0.22, 0.18) * drawn
    return jnp.clip(drawn, min=-bound, max=bound).astype(kind)


def noise_with(rng, dims, deviation, limit, shards, heavy, held_as=jnp.bfloat16):
    entries = deviation * jax.random.normal(rng, dims, jnp.float32)
    if shards:
        entries = entries * level_of(rng, dims, shards, -0.22, 0.18)
    return jnp.clip(spiked(entries, jax.random.fold_in(rng, 3), *heavy), -limit, limit).astype(held_as)


def setup_inputs(seed: int = 0) -> dict:
    streams_of = jax.random.split(jax.random.key(seed), 10)
    delta_query = noise_with(streams_of[0], (REPLICAS, LAYERS, D, QCOLS), 1.0, 6.0, ((0, 8), (3, 4)), (0, 2, 8, 2.0))
    master_query = gaussian(streams_of[1], (LAYERS, D, QCOLS), 0.5, 3.0, ((1, 8), (2, 4)), jnp.float32)
    moment_query = gaussian(streams_of[2], (LAYERS, D, QCOLS), 0.3, 3.0, ((1, 8), (2, 4)), jnp.float32)
    delta_latent = noise_with(streams_of[3], (REPLICAS, LAYERS, KV_RANK, KVCOLS), 1.0, 6.0, ((0, 8), (3, 4)), (0, 2, 8, 2.0))
    master_latent = gaussian(streams_of[4], (LAYERS, KV_RANK, KVCOLS), 0.5, 3.0, ((1, 8), (2, 4)), jnp.float32)
    moment_latent = gaussian(streams_of[5], (LAYERS, KV_RANK, KVCOLS), 0.3, 3.0, ((1, 8), (2, 4)), jnp.float32)
    delta_output = noise_with(streams_of[6], (REPLICAS, LAYERS, OROWS, D), 1.0, 6.0, ((0, 8), (2, 4)), (0, 3, 8, 2.0))
    master_output = gaussian(streams_of[7], (LAYERS, OROWS, D), 0.5, 3.0, ((1, 4), (2, 8)), jnp.float32)
    moment_output = gaussian(streams_of[8], (LAYERS, OROWS, D), 0.3, 3.0, ((1, 4), (2, 8)), jnp.float32)
    return dict(delta_query=delta_query, master_query=master_query, moment_query=moment_query, delta_latent=delta_latent, master_latent=master_latent, moment_latent=moment_latent, delta_output=delta_output, master_output=master_output, moment_output=moment_output)


OUTER_RATE = 0.7
OUTER_MOMENTUM = 0.9


def accumulate(delta):
    def add_replica(replica, running):
        return running + delta[replica].astype(jnp.float32)

    return lax.fori_loop(0, REPLICAS, add_replica, jnp.zeros(delta.shape[1:], jnp.float32))


def update(delta, master, moment):
    average = accumulate(delta) / REPLICAS
    momentum = OUTER_MOMENTUM * moment + average
    updated = master - OUTER_RATE * (average + OUTER_MOMENTUM * momentum)
    return updated.astype(jnp.bfloat16), updated, momentum


def reference(delta_query, master_query, moment_query, delta_latent, master_latent, moment_latent, delta_output, master_output, moment_output):
    query_params, query_master, query_moment = update(delta_query, master_query, moment_query)
    latent_params, latent_master, latent_moment = update(delta_latent, master_latent, moment_latent)
    output_params, output_master, output_moment = update(delta_output, master_output, moment_output)
    return (query_params, query_master, query_moment, latent_params, latent_master, latent_moment, output_params, output_master, output_moment)
```

```python
import functools

import jax
import jax.numpy as jnp
from jax import lax
from jax.experimental import pallas as pl
from jax.experimental.pallas import tpu as pltpu
from jax.sharding import PartitionSpec as P

OUTER_RATE = 0.7
OUTER_MOMENTUM = 0.9
MESH = pl.DeviceIdType.MESH
PIECE_BYTES = 32 * 1024
SPACING = 6
LEAD = 8


class Piece:
    def __init__(self, whole, own, first):
        self.layers, self.own_rows, self.cols = own
        self.by_rows = whole[1] != own[1]
        self.rows = 16
        while (
            self.own_rows % (2 * self.rows) == 0
            and 4 * self.rows * self.cols <= PIECE_BYTES
        ):
            self.rows *= 2
        self.per_layer = self.own_rows // self.rows
        self.first = first
        self.count = self.layers * self.per_layer

    def own(self, layer, row):
        return (layer, pl.ds(pl.multiple_of(row, 16), self.rows))

    def whole(self, layer, row, owner):
        if self.by_rows:
            start = pl.multiple_of(owner * self.own_rows + row, 16)
            return (layer, pl.ds(start, self.rows))
        start = pl.multiple_of(owner * self.cols, 128)
        return (layer, pl.ds(pl.multiple_of(row, 16), self.rows), pl.ds(start, self.cols))


def exchange(n, cuts, *refs):
    deltas, masters, moments = refs[0:9:3], refs[1:9:3], refs[2:9:3]
    params, new_masters, new_moments = refs[9:18:3], refs[10:18:3], refs[11:18:3]
    theirs, mine, up_in, down_in = refs[18:21], refs[21:24], refs[24:27], refs[27:30]
    (theirs_sem, mine_sem, up_sem, down_sem, gather_sem,
     master_sem, moment_sem, total_sem) = refs[30:]
    m = n // 2
    phases = (m + 1) // 2
    pieces = sum(cut.count for cut in cuts)
    me = lax.axis_index("rep")
    z, core = me // 2, me % 2
    partner = z * 2 + 1 - core
    above, below = (z + 1) * 2 + core, (z - 1) * 2 + core
    first, last = z == 0, z == m - 1

    def remote(src, dst, send, recv, rank):
        return pltpu.make_async_remote_copy(
            src_ref=src, dst_ref=dst, send_sem=send, recv_sem=recv,
            device_id={"rep": rank}, device_id_type=MESH,
        )

    def wait_bytes(ref, sem):
        pltpu.make_async_copy(ref, ref, sem).wait()

    def visit(i, act):
        for a, cut in enumerate(cuts):
            @pl.when((i >= cut.first) & (i < cut.first + cut.count))
            def _():
                k = i - cut.first
                layer = lax.div(k, cut.per_layer)
                act(a, cut, layer, (k - layer * cut.per_layer) * cut.rows)

    def chunks_of(s):
        phase = sum((s >= q * pieces).astype(jnp.int32) for q in range(1, phases))
        return phase, m - 1 - phase, s - phase * pieces

    def fetch(s):
        low, high, i = chunks_of(s)

        def act(a, cut, layer, row):
            here = cut.own(layer, row)

            def chunk(j):
                remote(
                    deltas[a].at[(0,) + cut.whole(layer, row, 2 * j + 1 - core)],
                    theirs[a].at[(j,) + here], total_sem.at[0, a], theirs_sem.at[j, i], partner,
                ).start()
                pltpu.make_async_copy(
                    deltas[a].at[(0,) + cut.whole(layer, row, 2 * j + core)],
                    mine[a].at[(j,) + here], mine_sem.at[j, i],
                ).start()

            chunk(high)

            @pl.when(low != high)
            def _():
                chunk(low)

            @pl.when((z == low) | (z == high))
            def _():
                pltpu.make_async_copy(masters[a].at[here], new_masters[a].at[here], master_sem.at[i]).start()
                pltpu.make_async_copy(moments[a].at[here], new_moments[a].at[here], moment_sem.at[i]).start()

        visit(i, act)

    def pair_sum(a, at, i):
        wait_bytes(theirs[a].at[at], theirs_sem.at[at[0], i])
        wait_bytes(mine[a].at[at], mine_sem.at[at[0], i])
        return theirs[a][at].astype(jnp.float32) + mine[a][at].astype(jnp.float32)

    def reduce(s, up):
        low, high, i = chunks_of(s)
        arrived, sem, target, starts = (up_in, up_sem, above, first) if up else (down_in, down_sem, below, last)

        def act(a, cut, layer, row):
            for j, other in ((high, low), (low, high)) if up else ((low, high), (high, low)):
                wanted = (j > z) if up else (j < z)
                if j is (low if up else high):
                    wanted = wanted & (j != other)
                at = (j,) + cut.own(layer, row)

                @pl.when(wanted & starts)
                def _():
                    mine[a][at] = pair_sum(a, at, i).astype(jnp.bfloat16)

                @pl.when(wanted & jnp.logical_not(starts))
                def _():
                    total = pair_sum(a, at, i)
                    wait_bytes(arrived[a].at[at], sem.at[j, i])
                    mine[a][at] = (total + arrived[a][at].astype(jnp.float32)).astype(jnp.bfloat16)

                @pl.when(wanted)
                def _():
                    remote(mine[a].at[at], arrived[a].at[at], total_sem.at[1, a], sem.at[j, i], target).start()

        visit(i, act)

    def hand_on(a, cut, layer, row, j, i, up, down):
        there = params[a].at[cut.whole(layer, row, 2 * j + core)]

        @pl.when(up)
        def _():
            remote(there, there, total_sem.at[4, a], gather_sem.at[j, i], above).start()

        @pl.when(down)
        def _():
            remote(there, there, total_sem.at[4, a], gather_sem.at[j, i], below).start()

        remote(there, there, total_sem.at[2, a], total_sem.at[3, a], partner).start()

    def update(i):
        def act(a, cut, layer, row):
            here = cut.own(layer, row)
            at = (z,) + here
            total = pair_sum(a, at, i)
            wait_bytes(new_masters[a].at[here], master_sem.at[i])
            wait_bytes(new_moments[a].at[here], moment_sem.at[i])

            @pl.when(z > 0)
            def _():
                wait_bytes(up_in[a].at[at], up_sem.at[z, i])

            @pl.when(z < m - 1)
            def _():
                wait_bytes(down_in[a].at[at], down_sem.at[z, i])

            def finish(summed):
                average = summed / n
                momentum = OUTER_MOMENTUM * new_moments[a][here] + average
                updated = new_masters[a][here] - OUTER_RATE * (average + OUTER_MOMENTUM * momentum)
                new_moments[a][here] = momentum
                new_masters[a][here] = updated
                params[a][cut.whole(layer, row, me)] = updated.astype(jnp.bfloat16)

            @pl.when(first)
            def _():
                finish(total + down_in[a][at].astype(jnp.float32))

            @pl.when(last)
            def _():
                finish(total + up_in[a][at].astype(jnp.float32))

            @pl.when(jnp.logical_not(first | last))
            def _():
                finish(total + up_in[a][at].astype(jnp.float32) + down_in[a][at].astype(jnp.float32))

            hand_on(a, cut, layer, row, z, i, z < m - 1, z > 0)

        visit(i, act)

    def gather(j, i):
        def act(a, cut, layer, row):
            wait_bytes(params[a].at[cut.whole(layer, row, 2 * j + core)], gather_sem.at[j, i])
            hand_on(a, cut, layer, row, j, i, (j < z) & (z < m - 1), (j > z) & (z > 0))

        visit(i, act)

    barrier = pltpu.get_barrier_semaphore()
    pl.semaphore_signal(barrier, inc=1, device_id={"rep": partner}, device_id_type=MESH)

    @pl.when(z > 0)
    def _():
        pl.semaphore_signal(barrier, inc=1, device_id={"rep": below}, device_id_type=MESH)

    @pl.when(z < m - 1)
    def _():
        pl.semaphore_signal(barrier, inc=1, device_id={"rep": above}, device_id_type=MESH)

    pl.semaphore_wait(barrier, 1 + (z > 0).astype(jnp.int32) + (z < m - 1).astype(jnp.int32))

    steps = phases * pieces
    lead = min(LEAD, steps)

    def early(s, carry):
        fetch(s)
        return carry

    lax.fori_loop(0, lead, early, 0)

    def tick(t, carry):
        @pl.when(t + lead < steps)
        def _():
            fetch(t + lead)

        for j in range(m):
            near = min(j, m - 1 - j)
            distance = jnp.where(z > j, z - j, j - z)
            i = t - near * pieces - SPACING * (m - 1 - near + distance)

            @pl.when((z != j) & (i >= 0) & (i < pieces))
            def _():
                gather(j, i)

        near = jnp.minimum(z, m - 1 - z)
        i = t - near * pieces - SPACING * (m - 1 - near)

        @pl.when((i >= 0) & (i < pieces))
        def _():
            update(i)

        up = t - SPACING * z

        @pl.when((z < m - 1) & (up >= 0) & (up < steps))
        def _():
            reduce(up, True)

        down = t - SPACING * (m - 1 - z)

        @pl.when((z > 0) & (down >= 0) & (down < steps))
        def _():
            reduce(down, False)

        return carry

    longest = max(
        near * pieces + SPACING * (m - 1 - near + max(j, m - 1 - j))
        for j in range(m)
        for near in [min(j, m - 1 - j)]
    )
    lax.fori_loop(0, longest + pieces, tick, 0)

    for a in range(len(cuts)):
        passed = theirs[a].at[pl.ds(0, m - 1)]
        wait_bytes(theirs[a], total_sem.at[0, a])
        wait_bytes(passed, total_sem.at[1, a])
        wait_bytes(theirs[a], total_sem.at[2, a])
        wait_bytes(theirs[a], total_sem.at[3, a])
        wait_bytes(theirs[a].at[0], total_sem.at[4, a])

        @pl.when(jnp.logical_not(first | last))
        def _():
            wait_bytes(theirs[a], total_sem.at[4, a])


def store(parts, *refs):
    count = len(refs) // 2
    held, out, sem = refs[:count], refs[count:2 * count], refs[2 * count]
    for a in range(count):
        for layer in range(held[a].shape[0]):
            pltpu.make_async_copy(held[a].at[layer], out[a].at[layer], sem.at[a]).start()
    for a in range(count):
        pltpu.make_async_copy(held[a], out[a], sem.at[a]).wait()


def on_device(n, *arrays):
    cuts, first = [], 0
    for delta, master in zip(arrays[0::3], arrays[1::3]):
        cut = Piece(delta.shape[1:], master.shape, first)
        cuts.append(cut)
        first += cut.count
    m = n // 2
    held, out_shape = [], []
    for delta, master in zip(arrays[0::3], arrays[1::3]):
        for shape, dtype in (
            (delta.shape[1:], jnp.bfloat16),
            (master.shape, jnp.float32),
            (master.shape, jnp.float32),
        ):
            held.append(pltpu.VMEM(shape, dtype))
            out_shape.append(jax.ShapeDtypeStruct(shape, dtype))
    anywhere = pl.BlockSpec(memory_space=pl.ANY)
    chunks = [pltpu.VMEM((m, *master.shape), jnp.bfloat16) for master in arrays[1::3]]
    flags = pltpu.SemaphoreType.DMA((m, first))
    results = pl.pallas_call(
        functools.partial(exchange, n, cuts),
        out_shape=held,
        in_specs=[anywhere] * len(arrays),
        out_specs=[pl.BlockSpec(memory_space=pltpu.VMEM)] * len(held),
        scratch_shapes=chunks * 4 + [flags] * 5
        + [pltpu.SemaphoreType.DMA((first,))] * 2 + [pltpu.SemaphoreType.DMA((5, len(cuts)))],
        compiler_params=pltpu.CompilerParams(
            collective_id=0, has_side_effects=True, vmem_limit_bytes=44 * 1024 * 1024
        ),
    )(*arrays)
    return tuple(
        pl.pallas_call(
            functools.partial(store, 1),
            out_shape=out_shape,
            in_specs=[anywhere] * len(out_shape),
            out_specs=[anywhere] * len(out_shape),
            scratch_shapes=[pltpu.SemaphoreType.DMA((len(out_shape),))],
            compiler_params=pltpu.CompilerParams(vmem_limit_bytes=1024 * 1024),
        )(*results)
    )


def solution(mesh):
    placed = (
        P("rep", None, None, "tp"),
        P(None, "rep", "tp"),
        P(None, "rep", "tp"),
        P("rep", None, None, "tp"),
        P(None, "rep", "tp"),
        P(None, "rep", "tp"),
        P("rep", None, "tp", None),
        P(None, "tp", "rep"),
        P(None, "tp", "rep"),
    )
    return jax.shard_map(
        functools.partial(on_device, mesh.shape["rep"]),
        mesh=mesh,
        in_specs=placed,
        out_specs=(
            P(None, None, "tp"),
            P(None, "rep", "tp"),
            P(None, "rep", "tp"),
            P(None, None, "tp"),
            P(None, "rep", "tp"),
            P(None, "rep", "tp"),
            P(None, "tp", None),
            P(None, "tp", "rep"),
            P(None, "tp", "rep"),
        ),
        check_vma=False,
    )
```
